32 devices in a mesh: row: 4 (over y, core), col: 8 (over z, x).
Axes of the slice: x: 2, y: 2, z: 4, core: 2. Of those that a mesh axis runs over, the one named last changes fastest.
Arguments:
- matrix: float32 [4096, 4096], P('row', 'col'), may hold values from -12 to 12, as said below
Outputs:
- sign_estimate: float32 [4096, 4096], P('row', 'col')
The draws below stay inside these ranges and needn't reach their ends.
Inputs may be any that keep to these rules, and one draw needn't show every extreme that they name: `matrix`: symmetric; the magnitudes of its eigenvalues, divided by the root mean square of all its eigenvalues, lie between 0.4 and 1.7.
All inputs are finite; a program needn't handle non-finite values.
Results may differ from the reference program's by a relative error of at most 0.0002.
Values sent between devices are 32-bit elements; how exact they have to be, the bound alone decides.
A program may use at most 64 MiB of HBM per device.

```python
import math
import jax
import jax.numpy as jnp
from jax import lax

N = 4096
ITERS = 2


def draw_matrix(key, part):
    keys = jax.random.split(jax.random.fold_in(key, 23), 4)
    mixing = 1.0
    factor_low = 0.9
    factor_high = 1.1
    scale_low = 0.25
    scale_high = 4.0
    rough = jax.random.normal(keys[0], (N, N), jnp.float32) * (mixing / math.sqrt(N))
    basis, upper = jnp.linalg.qr(jnp.eye(N, dtype=jnp.float32) + rough)
    place = jnp.arange(N, dtype=jnp.float32) / N
    factor = jax.random.uniform(keys[1], (N,), jnp.float32, factor_low, factor_high)
    signs = jax.random.rademacher(keys[2], (N,), jnp.float32)
    overall = jnp.exp(jax.random.uniform(keys[3], (), jnp.float32, math.log(scale_low), math.log(scale_high)))
    spectrum = signs * (0.6 + 0.9 * place) * factor * overall
    product = jnp.dot(basis * spectrum[None, :], basis.T, precision=lax.Precision.HIGHEST)
    return 0.5 * (product + product.T)


def setup_inputs(seed: int = 0) -> dict:
    arg_keys = jax.random.split(jax.random.key(seed), 2)
    matrix = draw_matrix(jax.random.fold_in(arg_keys[1], 71), 0)
    return dict(matrix=matrix)


def reference(matrix):
    total = jnp.sum(matrix * matrix)
    x_iter = matrix * jnp.sqrt(N / total)
    for step in range(ITERS):
        square = jnp.dot(x_iter.astype(jnp.float32), x_iter.astype(jnp.float32), preferred_element_type=jnp.float32, precision=lax.Precision.HIGHEST)
        cube_block = jnp.dot(x_iter.astype(jnp.float32), square.astype(jnp.float32), preferred_element_type=jnp.float32, precision=lax.Precision.HIGHEST)
        x_iter = 1.5 * x_iter - 0.5 * cube_block
    return x_iter
```

```python
import functools

import jax
import jax.numpy as jnp
from jax import lax
from jax.experimental import pallas as pl
from jax.experimental.pallas import tpu as pltpu
from jax.sharding import PartitionSpec as P

ITERS = 2
PIECES = 4
MESH = pl.DeviceIdType.MESH


class Gather:
    def __init__(self, axis, size, src, slot, line, pair, sends, copy_sem):
        self.axis, self.src, self.slot = axis, src, slot
        self.line, self.pair, self.sends, self.copy_sem = line, pair, sends, copy_sem
        me = lax.axis_index(axis)
        self.spots = size // 2
        self.spot, self.side = me // 2, lax.rem(me, 2)
        self.partner = me + 1 - 2 * self.side
        self.left, self.right = me - 2, me + 2
        self.pieces = PIECES
        self.depth = src.shape[0] // PIECES

    def ends(self):
        return ((self.left, self.spot > 0), (self.right, self.spot < self.spots - 1))

    def greet(self, barrier):
        pl.semaphore_signal(barrier, inc=1, device_id={self.axis: self.partner}, device_id_type=MESH)
        for target, there in self.ends():
            @pl.when(there)
            def _():
                pl.semaphore_signal(barrier, inc=1, device_id={self.axis: target}, device_id_type=MESH)

    def peers(self):
        return 1 + sum(there.astype(jnp.int32) for _, there in self.ends())

    def part(self, ref, piece):
        return ref.at[pl.ds(piece * self.depth, self.depth), :]

    def copy(self, spot, piece, way, own):
        dst = self.part(self.slot(2 * spot + self.side), piece)
        src = self.part(self.src, piece) if own else dst
        sems = self.pair if way == 2 else self.line
        target = (self.left, self.right, self.partner)[way]
        return pltpu.make_async_remote_copy(
            src_ref=src, dst_ref=dst, send_sem=self.sends.at[way, spot, piece], recv_sem=sems.at[spot, piece],
            device_id={self.axis: target}, device_id_type=MESH)

    def arrive(self, spot, piece, side, sems):
        dst = self.part(self.slot(2 * spot + side), piece)
        pltpu.make_async_remote_copy(
            src_ref=dst, dst_ref=dst, send_sem=self.sends.at[2, spot, piece], recv_sem=sems.at[spot, piece],
            device_id={self.axis: self.partner}, device_id_type=MESH).wait_recv()

    def begin(self):
        self.keep = pltpu.make_async_copy(self.src, self.slot(2 * self.spot + self.side), self.copy_sem)
        self.keep.start()
        for piece in range(self.pieces):
            for way, (_, there) in enumerate(self.ends()):
                @pl.when(there)
                def _():
                    self.copy(self.spot, piece, way, True).start()
            self.copy(self.spot, piece, 2, True).start()

    def relay(self, far, piece):
        for way, spot in ((0, self.spot + far), (1, self.spot - far)):
            here = spot < self.spots if way == 0 else spot >= 0
            @pl.when(here)
            def _():
                self.arrive(spot, piece, self.side, self.line)
                @pl.when(self.ends()[way][1])
                def _():
                    self.copy(spot, piece, way, False).start()
                self.copy(spot, piece, 2, False).start()

    def finish(self):
        self.keep.wait()
        for far in range(self.spots):
            for piece in range(self.pieces):
                if far == 0:
                    self.arrive(self.spot, piece, 1 - self.side, self.pair)
                    for way, (_, there) in enumerate(self.ends()):
                        @pl.when(there)
                        def _():
                            self.copy(self.spot, piece, way, True).wait_send()
                    self.copy(self.spot, piece, 2, True).wait_send()
                    continue
                for way, spot in ((0, self.spot + far), (1, self.spot - far)):
                    here = spot < self.spots if way == 0 else spot >= 0
                    @pl.when(here)
                    def _():
                        self.arrive(spot, piece, 1 - self.side, self.pair)
                        @pl.when(self.ends()[way][1])
                        def _():
                            self.copy(spot, piece, way, False).wait_send()
                        self.copy(spot, piece, 2, False).wait_send()


def run_gathers(gathers):
    barrier = pltpu.get_barrier_semaphore()
    for g in gathers:
        g.greet(barrier)
    pl.semaphore_wait(barrier, sum(g.peers() for g in gathers))
    for g in gathers:
        g.begin()
    for far in range(1, max(g.spots for g in gathers)):
        for piece in range(PIECES):
            for g in gathers:
                if far < g.spots:
                    g.relay(far, piece)
    for g in gathers:
        g.finish()


def both_kernel(row_n, col_n, x_ref, rows_ref, cols_ref, line_c, pair_c, sends_c, line_r, pair_r, sends_r, copies):
    depth, width = x_ref.shape
    rows_slot = lambda i: rows_ref.at[:, pl.ds(pl.multiple_of(i * width, width), width)]
    cols_slot = lambda i: cols_ref.at[pl.ds(pl.multiple_of(i * depth, depth), depth), :]
    run_gathers((
        Gather("row", row_n, x_ref, cols_slot, line_r, pair_r, sends_r, copies.at[1]),
        Gather("col", col_n, x_ref, rows_slot, line_c, pair_c, sends_c, copies.at[0]),
    ))


def cols_kernel(row_n, x_ref, cols_ref, line_r, pair_r, sends_r, copies):
    depth = x_ref.shape[0]
    cols_slot = lambda i: cols_ref.at[pl.ds(pl.multiple_of(i * depth, depth), depth), :]
    run_gathers((Gather("row", row_n, x_ref, cols_slot, line_r, pair_r, sends_r, copies.at[0]),))


def sems(size):
    dma = pltpu.SemaphoreType.DMA
    return [dma((size // 2, PIECES)), dma((size // 2, PIECES)), dma((3, size // 2, PIECES))]


ANY = pl.BlockSpec(memory_space=pl.ANY)


def gather_both(x, row_n, col_n):
    depth, width = x.shape
    return pl.pallas_call(
        functools.partial(both_kernel, row_n, col_n),
        out_shape=(jax.ShapeDtypeStruct((depth, width * col_n), x.dtype),
                   jax.ShapeDtypeStruct((depth * row_n, width), x.dtype)),
        in_specs=[ANY], out_specs=(ANY, ANY),
        scratch_shapes=sems(col_n) + sems(row_n) + [pltpu.SemaphoreType.DMA((2,))],
        compiler_params=pltpu.CompilerParams(collective_id=0, has_side_effects=True),
        name="gather_both",
    )(x)


def gather_cols(x, row_n):
    depth, width = x.shape
    return pl.pallas_call(
        functools.partial(cols_kernel, row_n),
        out_shape=jax.ShapeDtypeStruct((depth * row_n, width), x.dtype),
        in_specs=[ANY], out_specs=ANY,
        scratch_shapes=sems(row_n) + [pltpu.SemaphoreType.DMA((1,))],
        compiler_params=pltpu.CompilerParams(collective_id=1, has_side_effects=True),
        name="gather_cols",
    )(x)


def dot(a, b):
    return jnp.dot(a, b, preferred_element_type=jnp.float32, precision=lax.Precision.HIGH)


def shards(row_n, col_n, matrix):
    depth = matrix.shape[0]
    factor = jnp.sqrt(depth * row_n / lax.psum(jnp.sum(matrix * matrix), ("row", "col")))
    x_iter = matrix
    for step in range(ITERS):
        rows_panel, cols_panel = gather_both(x_iter, row_n, col_n)
        square = dot(rows_panel, cols_panel)
        cube = dot(rows_panel, gather_cols(square, row_n))
        if step == 0:
            x_iter = factor * (1.5 * x_iter - (0.5 * factor * factor) * cube)
        else:
            x_iter = 1.5 * x_iter - 0.5 * cube
    return x_iter


def solution(mesh):
    body = functools.partial(shards, mesh.shape["row"], mesh.shape["col"])
    return jax.shard_map(body, mesh=mesh, in_specs=(P("row", "col"),), out_specs=P("row", "col"), check_vma=False)
```

```python
import functools

import jax
import jax.numpy as jnp
from jax import lax
from jax.experimental import pallas as pl
from jax.experimental.pallas import tpu as pltpu
from jax.sharding import PartitionSpec as P

ITERS = 2
PIECES = 8
MESH = pl.DeviceIdType.MESH


class Gather:
    def __init__(self, axis, size, src, slot, line, pair, sends, copy_sem, swapped=0):
        self.axis, self.src, self.slot = axis, src, slot
        self.line, self.pair, self.sends, self.copy_sem = line, pair, sends, copy_sem
        me = lax.axis_index(axis)
        self.spots = size // 2
        self.spot, self.side = me // 2, lax.rem(me, 2)
        self.partner = me + 1 - 2 * self.side
        self.left, self.right = me - 2, me + 2
        self.pieces = line.shape[1]
        self.depth = src.shape[0] // self.pieces
        self.swapped = swapped

    def ends(self):
        return ((self.left, self.spot > 0), (self.right, self.spot < self.spots - 1))

    def greet(self, barrier):
        pl.semaphore_signal(barrier, inc=1, device_id={self.axis: self.partner}, device_id_type=MESH)
        for target, there in self.ends():
            @pl.when(there)
            def _():
                pl.semaphore_signal(barrier, inc=1, device_id={self.axis: target}, device_id_type=MESH)

    def peers(self):
        return 1 + sum(there.astype(jnp.int32) for _, there in self.ends())

    def part(self, ref, piece):
        return ref.at[pl.ds(piece * self.depth, self.depth), :]

    def copy(self, spot, piece, way, own, other=False):
        side = 1 - self.side if other else self.side
        dst = self.part(self.slot(2 * spot + side), piece)
        src = self.part(self.src, piece) if own else dst
        sems = self.pair if way == 2 or other else self.line
        target = (self.left, self.right, self.partner)[way]
        return pltpu.make_async_remote_copy(
            src_ref=src, dst_ref=dst, send_sem=self.sends.at[way + 3 * other, spot, piece],
            recv_sem=sems.at[spot, piece], device_id={self.axis: target}, device_id_type=MESH)

    def arrive(self, spot, piece, side, sems):
        dst = self.part(self.slot(2 * spot + side), piece)
        pltpu.make_async_remote_copy(
            src_ref=dst, dst_ref=dst, send_sem=self.sends.at[2, spot, piece], recv_sem=sems.at[spot, piece],
            device_id={self.axis: self.partner}, device_id_type=MESH).wait_recv()

    def onward(self, act, spot, piece, ways, own, other=False):
        for way in ways:
            @pl.when(self.ends()[way][1])
            def _():
                getattr(self.copy(spot, piece, way, own, other), act)()

    def far_spots(self, far):
        return ((0, self.spot + far, self.spot + far < self.spots), (1, self.spot - far, self.spot >= far))

    def begin(self):
        self.keep = pltpu.make_async_copy(self.src, self.slot(2 * self.spot + self.side), self.copy_sem)
        self.keep.start()
        for piece in range(self.pieces):
            self.copy(self.spot, piece, 2, True).start()
            self.onward("start", self.spot, piece, (0, 1), True)

    def cross(self):
        for piece in range(self.swapped):
            self.arrive(self.spot, piece, 1 - self.side, self.pair)
            self.onward("start", self.spot, piece, (0, 1), False, True)

    def relay(self, far, piece):
        for way, spot, here in self.far_spots(far):
            @pl.when(here)
            def _():
                self.arrive(spot, piece, self.side, self.line)
                self.onward("start", spot, piece, (way,), False)
                if piece >= self.swapped:
                    self.copy(spot, piece, 2, False).start()

    def relay_crossed(self, far):
        for piece in range(self.swapped):
            for way, spot, here in self.far_spots(far):
                @pl.when(here)
                def _():
                    self.arrive(spot, piece, 1 - self.side, self.pair)
                    self.onward("start", spot, piece, (way,), False, True)

    def finish(self):
        self.keep.wait()
        for piece in range(self.pieces):
            crossed = piece < self.swapped
            if not crossed:
                self.arrive(self.spot, piece, 1 - self.side, self.pair)
            self.copy(self.spot, piece, 2, True).wait_send()
            self.onward("wait_send", self.spot, piece, (0, 1), True)
            if crossed:
                self.onward("wait_send", self.spot, piece, (0, 1), False, True)
        for far in range(1, self.spots):
            for piece in range(self.pieces):
                crossed = piece < self.swapped
                for way, spot, here in self.far_spots(far):
                    @pl.when(here)
                    def _():
                        if not crossed:
                            self.arrive(spot, piece, 1 - self.side, self.pair)
                            self.copy(spot, piece, 2, False).wait_send()
                        self.onward("wait_send", spot, piece, (way,), False)
                        if crossed:
                            self.onward("wait_send", spot, piece, (way,), False, True)


def run_gathers(gathers):
    barrier = pltpu.get_barrier_semaphore()
    for g in gathers:
        g.greet(barrier)
    pl.semaphore_wait(barrier, sum(g.peers() for g in gathers))
    for g in gathers:
        g.begin()
    for g in gathers:
        g.cross()
    for far in range(1, max(g.spots for g in gathers)):
        for piece in range(PIECES):
            for g in gathers:
                if far < g.spots and piece < g.pieces:
                    g.relay(far, piece)
        for g in gathers:
            if far < g.spots:
                g.relay_crossed(far)
    for g in gathers:
        g.finish()


def down(ref, depth):
    return lambda i: ref.at[pl.ds(pl.multiple_of(i * depth, depth), depth), :]


def across(ref, width):
    return lambda i: ref.at[:, pl.ds(pl.multiple_of(i * width, width), width)]


def both_kernel(row_n, col_n, x_ref, s_ref, rows_ref, cols_ref, stats_ref, *sems):
    depth, width = x_ref.shape
    copies = sems[9]
    run_gathers((
        Gather("col", col_n, s_ref, down(stats_ref, 8), *sems[6:9], copies.at[2]),
        Gather("row", row_n, x_ref, down(cols_ref, depth), *sems[3:6], copies.at[1]),
        Gather("col", col_n, x_ref, across(rows_ref, width), *sems[0:3], copies.at[0], swapped=1),
    ))


def cols_kernel(row_n, x_ref, s_ref, cols_ref, stats_ref, *sems):
    depth = x_ref.shape[0]
    copies = sems[6]
    run_gathers((
        Gather("row", row_n, s_ref, down(stats_ref, 8), *sems[3:6], copies.at[1]),
        Gather("row", row_n, x_ref, down(cols_ref, depth), *sems[0:3], copies.at[0]),
    ))


def sems(size, pieces):
    dma = pltpu.SemaphoreType.DMA
    return [dma((size // 2, pieces)), dma((size // 2, pieces)), dma((5, size // 2, pieces))]


ANY = pl.BlockSpec(memory_space=pl.ANY)


def gather_both(x, stat, row_n, col_n):
    depth, width = x.shape
    return pl.pallas_call(
        functools.partial(both_kernel, row_n, col_n),
        out_shape=(jax.ShapeDtypeStruct((depth, width * col_n), x.dtype),
                   jax.ShapeDtypeStruct((depth * row_n, width), x.dtype),
                   jax.ShapeDtypeStruct((8 * col_n, 128), x.dtype)),
        in_specs=[ANY, ANY], out_specs=(ANY, ANY, ANY),
        scratch_shapes=sems(col_n, PIECES) + sems(row_n, PIECES) + sems(col_n, 1) + [pltpu.SemaphoreType.DMA((3,))],
        compiler_params=pltpu.CompilerParams(collective_id=0, has_side_effects=True),
        name="gather_both",
    )(x, stat)


def gather_cols(x, stat, row_n):
    depth, width = x.shape
    return pl.pallas_call(
        functools.partial(cols_kernel, row_n),
        out_shape=(jax.ShapeDtypeStruct((depth * row_n, width), x.dtype),
                   jax.ShapeDtypeStruct((8 * row_n, 128), x.dtype)),
        in_specs=[ANY, ANY], out_specs=(ANY, ANY),
        scratch_shapes=sems(row_n, PIECES) + sems(row_n, 1) + [pltpu.SemaphoreType.DMA((2,))],
        compiler_params=pltpu.CompilerParams(collective_id=1, has_side_effects=True),
        name="gather_cols",
    )(x, stat)


def dot(a, b):
    return jnp.dot(a, b, preferred_element_type=jnp.float32, precision=lax.Precision.HIGH)


def fold(x):
    return jnp.sum(x.reshape(x.shape[0] // 8, 8, x.shape[1] // 128, 128), axis=(0, 2))


def shards(row_n, col_n, matrix):
    x_iter = matrix
    stat = fold(matrix * matrix)
    for step in range(ITERS):
        rows_panel, cols_panel, stats = gather_both(x_iter, stat, row_n, col_n)
        square = dot(rows_panel, cols_panel)
        square_panel, stats = gather_cols(square, fold(stats), row_n)
        cube = dot(rows_panel, square_panel)
        if step == 0:
            factor = jnp.sqrt(matrix.shape[0] * row_n / jnp.sum(stats))
            x_iter = factor * (1.5 * x_iter - (0.5 * factor * factor) * cube)
        else:
            x_iter = 1.5 * x_iter - 0.5 * cube
    return x_iter


def solution(mesh):
    body = functools.partial(shards, mesh.shape["row"], mesh.shape["col"])
    return jax.shard_map(body, mesh=mesh, in_specs=(P("row", "col"),), out_specs=P("row", "col"), check_vma=False)
```
